32 devices in a mesh: seq: 8 (over z, y), grp: 4 (over x, core).
Axes of the slice: x: 2, y: 2, z: 4, core: 2. Of those that a mesh axis runs over, the one named last changes fastest.
Arguments:
- hidden: bfloat16 [256, 8192], P('grp', 'seq'), may hold values from -6 to 6
- w_qkv: bfloat16 [8192, 10240], P('seq', 'grp'), may hold values from -0.0625 to 0.0625
- b_qkv: float32 [10240], P('grp'), may hold values from -3 to 3
- w_out: bfloat16 [8192, 8192], P('seq', 'grp'), may hold values from -0.0625 to 0.0625
- k_cache: bfloat16 [4, 32768, 1024], P('grp', 'seq'), may hold values from -600 to 600
- v_cache: bfloat16 [4, 32768, 1024], P('grp', 'seq'), may hold values from -6 to 6
- lengths: int32 [256], replicated, may hold values from 1 to 16384, as said below
- page_table: int32 [256, 128], replicated, may hold values from -1 to 255, as said below
- positions: int32 [3, 256], replicated, may hold values from 0 to 4095
- group_of: int32 [256], replicated, may hold values from 0 to 3, as said below
Outputs:
- mixed: bfloat16 [256, 8192], P('seq', 'grp')
The draws below stay inside these ranges and needn't reach their ends.
Inputs may be any that keep to these rules, and one draw needn't show every extreme that they name: `group_of`: each group serves exactly 64 requests. `lengths`: each group has a request of exactly 16384 cached positions. `page_table`: entry j of row r is the page of request r's group pool (page p lies on that group's device p // 32 of seq) that holds its positions j * 128 to (j + 1) * 128 - 1, for j < ceil(lengths[r] / 128); later entries are -1; no page belongs to two requests.
All inputs are finite; a program needn't handle non-finite values.
Results may differ from the reference program's by a relative error of at most 0.015.
The reference program's roundings to bfloat16 on the way count: a program that leaves them out, or rounds other values in their place, can miss the bound.
Values may be sent and summed in bfloat16 or wider, within the bound.
A program may use at most 128 MiB of HBM per device.

```python
import math
import jax
import jax.numpy as jnp
from jax import lax

D = 8192
HQ = 64
KVH = 8
HD = 128
REQ_GRP = 64
POOL = 32
PAGE = 128
QKV = 10240
MAXP = 128
REQ = 256
N_SEQ = 8
N_GRP = 4


def layout(key):
    base_key = jax.random.fold_in(key, 4242)
    key_group, key_weight, key_tail, key_place = jax.random.split(base_key, 4)
    group_pages = N_SEQ * POOL
    group_of = (jax.random.permutation(key_group, REQ).astype(jnp.int32) // REQ_GRP).astype(jnp.int32)
    served_order = jnp.argsort(group_of, stable=True).astype(jnp.int32)
    rank_of = jnp.zeros((REQ,), jnp.int32).at[served_order].set(jnp.arange(REQ, dtype=jnp.int32))
    leading = rank_of % REQ_GRP == 0
    exponent = jax.random.randint(key_weight, (REQ,), 0, 5).astype(jnp.int32)
    weight = jnp.left_shift(jnp.ones((REQ,), jnp.int32), exponent)
    member = group_of[:, None] == jnp.arange(N_GRP, dtype=jnp.int32)[None, :]
    group_weight = jnp.sum(jnp.where(member, weight[:, None], 0), axis=0).astype(jnp.int32)
    spare_pages = group_pages // 2 - REQ_GRP
    page_counts = 1 + spare_pages * weight // group_weight[group_of]
    page_counts = jnp.where(leading, MAXP, jnp.minimum(page_counts, MAXP)).astype(jnp.int32)
    tail_fill = jax.random.randint(key_tail, (REQ,), 1, PAGE + 1).astype(jnp.int32)
    lengths = (page_counts - 1) * PAGE + jnp.where(leading, PAGE, tail_fill)
    sorted_pages = page_counts[served_order].reshape(N_GRP, REQ_GRP)
    starts_sorted = (jnp.cumsum(sorted_pages, axis=1) - sorted_pages).reshape(REQ)
    starts = starts_sorted[rank_of]
    device_of = jnp.arange(group_pages, dtype=jnp.int32) // POOL
    priority = jax.random.randint(key_place, (N_GRP, group_pages), 0, 4096).astype(jnp.int32)
    priority = priority + device_of[None, :] * (6144 // N_SEQ)
    priority = priority * group_pages + jnp.arange(group_pages, dtype=jnp.int32)[None, :]
    placed = jnp.argsort(priority, axis=1).astype(jnp.int32)
    logical = jnp.arange(MAXP, dtype=jnp.int32)
    slot_index = jnp.minimum(starts[:, None] + logical[None, :], group_pages - 1)
    physical = placed[group_of[:, None], slot_index]
    page_table = jnp.where(logical[None, :] < page_counts[:, None], physical, -1)
    return (group_of.astype(jnp.int32), lengths.astype(jnp.int32), page_table.astype(jnp.int32))


def draw_group_of(key, part):
    return layout(key)[0]


def draw_lengths(key, part):
    return layout(key)[1]


def draw_page_table(key, part):
    return layout(key)[2]


def draw_k_cache(key, part):
    extent = (N_GRP, N_SEQ * POOL * PAGE, KVH * HD)
    drawn_keys = jnp.clip(jax.random.normal(jax.random.fold_in(key, 11), extent, jnp.float32), -6.0, 6.0)
    return drawn_keys.astype(jnp.bfloat16)


def touch_ends(drawn, stream_key, least, largest):
    place = [jax.random.randint(jax.random.fold_in(stream_key, axis), (), 0, length) for axis, length in enumerate(drawn.shape)]
    longest = drawn.shape.index(max(drawn.shape))
    next_to = place[:longest] + [(place[longest] + 1) % drawn.shape[longest]] + place[longest + 1:]
    return drawn.at[tuple(place)].set(least).at[tuple(next_to)].set(largest)


def shard_levels(stream_key, shape, cuts, low, high):
    def one(position, shards_of):
        draws = jax.random.uniform(jax.random.fold_in(jax.random.fold_in(stream_key, 6), position), (shards_of,), jnp.float32, low / len(cuts), high / len(cuts))
        return jnp.repeat(jnp.exp(draws), shape[position] // shards_of).reshape((-1,) + (1,) * (len(shape) - position - 1))

    factor_of = one(*cuts[0])
    for cut in cuts[1:]:
        factor_of = factor_of * one(*cut)
    return factor_of


def scatter_about(own_key, shape, width, most, shards=(), kind=jnp.bfloat16):
    result = jax.random.normal(own_key, shape, jnp.float32) * width
    if len(shards) > 0:
        result = shard_levels(own_key, shape, shards, -0.22, 0.18) * result
    return jnp.clip(result, min=-most, max=most).astype(kind)


def setup_inputs(seed: int = 0) -> dict:
    arg_keys = jax.random.split(jax.random.key(seed), 11)
    return {
        "hidden": scatter_about(arg_keys[0], (REQ, D), 1.0, 6.0, ((0, 4), (1, 8))),
        "w_qkv": scatter_about(arg_keys[1], (D, QKV), D ** -0.5, 0.0625, ((0, 8), (1, 4))),
        "b_qkv": scatter_about(arg_keys[2], (QKV,), 0.5, 3.0, ((0, 4),), jnp.float32),
        "w_out": scatter_about(arg_keys[3], (HQ * HD, D), (HQ * HD) ** -0.5, 0.0625, ((0, 8), (1, 4))),
        "k_cache": draw_k_cache(jax.random.fold_in(arg_keys[10], 71), 0),
        "v_cache": scatter_about(arg_keys[5], (N_GRP, N_SEQ * POOL * PAGE, KVH * HD), 1.0, 6.0, ((0, 4), (1, 8))),
        "lengths": draw_lengths(jax.random.fold_in(arg_keys[10], 71), 0),
        "page_table": draw_page_table(jax.random.fold_in(arg_keys[10], 71), 0),
        "positions": touch_ends(jax.random.randint(arg_keys[8], (3, REQ), 0, 4096), jax.random.fold_in(arg_keys[8], 1), 0, 4095).astype(jnp.int32),
        "group_of": draw_group_of(jax.random.fold_in(arg_keys[10], 71), 0),
    }


rope_base = 1000000.0
neg_fill = -1.0e30


def rotate_heads(values, places, col_start, head_dim, turned):
    row_count, col_count = values.shape
    columns = col_start + jnp.arange(col_count, dtype=jnp.int32)
    within = columns % head_dim
    freq_index = within % (head_dim // 2)
    inverse_freq = jnp.exp(freq_index.astype(jnp.float32) * (-2.0 * math.log(rope_base) / head_dim))
    section = jnp.where(freq_index < head_dim // 8, 0, jnp.where(freq_index < head_dim // 8 + 3 * head_dim // 16, 1, 2))
    place_float = places.astype(jnp.float32)
    chosen = jnp.where(section[None, :] == 0, place_float[0][:, None],
                       jnp.where(section[None, :] == 1, place_float[1][:, None], place_float[2][:, None]))
    angles = chosen * inverse_freq[None, :]
    halves = values.reshape(row_count, col_count // head_dim, 2, head_dim // 2)
    partner = jnp.concatenate([-halves[:, :, 1:], halves[:, :, :1]], axis=2).reshape(row_count, col_count)
    rotated = values * jnp.cos(angles) + partner * jnp.sin(angles)
    return jnp.where((columns < turned)[None, :], rotated, values)


def reference(hidden, w_qkv, b_qkv, w_out, k_cache, v_cache, lengths, page_table, positions, group_of):
    turned = (HQ + KVH) * HD
    group_q = HQ // KVH
    score_scale = HD ** -0.5
    projected = jnp.dot(hidden, w_qkv, preferred_element_type=jnp.float32) + b_qkv[None, :]
    fresh_rows = rotate_heads(projected, positions, 0, HD, turned).astype(jnp.bfloat16)
    query_rows = fresh_rows[:, : HQ * HD]
    key_new = fresh_rows[:, HQ * HD: turned]
    value_new = fresh_rows[:, turned:]
    group_pages = N_SEQ * POOL
    all_pages = N_GRP * group_pages
    page_counts = (lengths + PAGE - 1) // PAGE
    logical = jnp.arange(MAXP, dtype=jnp.int32)
    usable = logical[None, :] < page_counts[:, None]
    target = jnp.where(usable, group_of[:, None] * group_pages + page_table, all_pages).reshape(-1).astype(jnp.int32)
    page_owner = jnp.full((all_pages,), -1, jnp.int32).at[target].set(
        jnp.repeat(jnp.arange(REQ, dtype=jnp.int32), MAXP), mode="drop")
    page_number = jnp.zeros((all_pages,), jnp.int32).at[target].set(jnp.tile(logical, REQ), mode="drop")
    block_count = all_pages // POOL

    def one_block(block_items):
        key_block, value_block, owner_block, number_block = block_items
        present = owner_block >= 0
        holder = jnp.maximum(owner_block, 0)
        page_query = query_rows[holder].astype(jnp.float32).reshape(POOL, KVH, group_q, HD)
        scores = jnp.einsum("pkgd,ptkd->pkgt", page_query, key_block.astype(jnp.float32),
                            precision=lax.Precision.HIGHEST) * score_scale
        places_in = number_block[:, None] * PAGE + jnp.arange(PAGE, dtype=jnp.int32)[None, :]
        alive_rows = present[:, None] & (places_in < lengths[holder][:, None])
        alive_wide = alive_rows[:, None, None, :]
        page_max = jnp.max(jnp.where(alive_wide, scores, neg_fill), axis=3)
        weights = jnp.exp(jnp.where(alive_wide, scores - page_max[..., None], neg_fill))
        page_total = jnp.sum(weights, axis=3)
        rounded = weights.astype(jnp.bfloat16).astype(jnp.float32)
        page_out = jnp.einsum("pkgt,ptkd->pkgd", rounded, value_block.astype(jnp.float32),
                              precision=lax.Precision.HIGHEST)
        return page_max.reshape(POOL, HQ), page_total.reshape(POOL, HQ), page_out.reshape(POOL, HQ * HD)

    page_max, page_total, page_out = lax.map(one_block, (
        k_cache.reshape(block_count, POOL, PAGE, KVH, HD),
        v_cache.reshape(block_count, POOL, PAGE, KVH, HD),
        page_owner.reshape(block_count, POOL),
        page_number.reshape(block_count, POOL)))
    page_max = page_max.reshape(all_pages, HQ)
    page_total = page_total.reshape(all_pages, HQ)
    page_out = page_out.reshape(all_pages, HQ, HD)
    segment = jnp.where(page_owner >= 0, page_owner, REQ).astype(jnp.int32)
    new_score = jnp.einsum("rkgd,rkd->rkg", query_rows.astype(jnp.float32).reshape(REQ, KVH, group_q, HD),
                           key_new.astype(jnp.float32).reshape(REQ, KVH, HD),
                           precision=lax.Precision.HIGHEST).reshape(REQ, HQ) * score_scale
    page_peak = jnp.full((REQ + 1, HQ), neg_fill, jnp.float32).at[segment].max(page_max)
    peak_score = jnp.maximum(page_peak[:REQ], new_score)
    peak_wide = jnp.concatenate([peak_score, jnp.zeros((1, HQ), jnp.float32)], axis=0)
    factor = jnp.where((page_owner >= 0)[:, None], jnp.exp(page_max - peak_wide[segment]), 0.0)
    summed_total = jax.ops.segment_sum(page_total * factor, segment, REQ + 1)[:REQ]
    summed_out = jax.ops.segment_sum(page_out * factor[..., None], segment, REQ + 1)[:REQ]
    fresh_weight = jnp.exp(new_score - peak_score)
    value_heads = jnp.broadcast_to(value_new.astype(jnp.float32).reshape(REQ, KVH, 1, HD),
                                   (REQ, KVH, group_q, HD)).reshape(REQ, HQ, HD)
    numerator = summed_out + fresh_weight[..., None] * value_heads
    denominator = summed_total + fresh_weight
    attended = (numerator / denominator[..., None]).reshape(REQ, HQ * HD).astype(jnp.bfloat16)
    return jnp.dot(attended, w_out, preferred_element_type=jnp.float32).astype(jnp.bfloat16)
```

```python
import functools
import math

import jax
import jax.numpy as jnp
from jax import lax
from jax.experimental import pallas as pl
from jax.experimental.pallas import tpu as pltpu
from jax.sharding import PartitionSpec as P

HQ = 64
KVH = 8
HD = 128
PAGE = 128


rope_base = 1000000.0
neg_fill = -1e30


def rotate_heads(values, places, col_start, head_dim, turned):
    row_count, col_count = values.shape
    columns = col_start + jnp.arange(col_count, dtype=jnp.int32)
    within = columns % head_dim
    freq_index = within % (head_dim // 2)
    inverse_freq = jnp.exp(freq_index.astype(jnp.float32) * (-2.0 * math.log(rope_base) / head_dim))
    section = jnp.where(
        freq_index < head_dim // 8,
        0,
        jnp.where(freq_index < head_dim // 8 + 3 * head_dim // 16, 1, 2),
    )
    place_float = places.astype(jnp.float32)
    chosen = jnp.where(
        section[None, :] == 0,
        place_float[0][:, None],
        jnp.where(section[None, :] == 1, place_float[1][:, None], place_float[2][:, None]),
    )
    angles = chosen * inverse_freq[None, :]
    halves = values.reshape(row_count, col_count // head_dim, 2, head_dim // 2)
    partner = jnp.concatenate([-halves[:, :, 1:], halves[:, :, :1]], axis=2).reshape(
        row_count, col_count
    )
    rotated = values * jnp.cos(angles) + partner * jnp.sin(angles)
    return jnp.where((columns < turned)[None, :], rotated, values)


def attend_pages(block_pages, owner_ref, live_ref, rows_ref, key_ref, value_ref, out_ref, stat_ref):
    step = pl.program_id(0)
    group_q = HQ // KVH
    width = KVH * HD

    @pl.when(step == 0)
    def _():
        out_ref[...] = jnp.zeros_like(out_ref)
        lanes = lax.broadcasted_iota(jnp.int32, stat_ref.shape, 2)
        stat_ref[...] = jnp.where(lanes < HD // 2, neg_fill, 0.0)

    row_head = lax.broadcasted_iota(jnp.int32, (HQ, width), 0) // group_q
    col_head = lax.broadcasted_iota(jnp.int32, (HQ, width), 1) // HD
    own_head = (row_head == col_head).astype(jnp.float32).astype(jnp.bfloat16)
    place = lax.broadcasted_iota(jnp.int32, (HQ, PAGE), 1)
    lane = lax.broadcasted_iota(jnp.int32, (HQ, HD), 1)
    pages = []
    for j in range(block_pages):
        owner = owner_ref[step * block_pages + j]
        alive = place < live_ref[step * block_pages + j]
        query = rows_ref[owner, :HQ, :]
        spread = jnp.concatenate([query] * KVH, axis=1) * own_head
        keys = key_ref[0, j * PAGE : (j + 1) * PAGE, :]
        values = value_ref[0, j * PAGE : (j + 1) * PAGE, :]
        scores = lax.dot_general(
            spread, keys, (((1,), (1,)), ((), ())), preferred_element_type=jnp.float32
        ) * (HD**-0.5)
        scores = jnp.where(alive, scores, neg_fill)
        page_max = jnp.max(scores, axis=1, keepdims=True)
        weights = jnp.where(alive, jnp.exp(scores - page_max), 0.0)
        page_total = jnp.sum(weights, axis=1, keepdims=True)
        wide = jnp.dot(weights.astype(jnp.bfloat16), values, preferred_element_type=jnp.float32)
        page_out = jnp.concatenate(
            [
                wide[h * group_q : (h + 1) * group_q, h * HD : (h + 1) * HD]
                for h in range(KVH)
            ],
            axis=0,
        )
        pages.append((owner, page_max, page_total, page_out))
    for owner, page_max, page_total, page_out in pages:
        stat = stat_ref[owner]
        old_max = stat[:, :1]
        new_max = jnp.maximum(old_max, page_max)
        kept = jnp.exp(old_max - new_max)
        added = jnp.exp(page_max - new_max)
        out_ref[owner] = out_ref[owner] * kept + page_out * added
        total = stat[:, HD // 2 : HD // 2 + 1] * kept + page_total * added
        stat_ref[owner] = jnp.where(lane < HD // 2, new_max, total)


def local_attention(owner, live, rows, k_cache, v_cache):
    group_size = rows.shape[0]
    pool_pages = k_cache.shape[1] // PAGE
    block_pages = math.gcd(pool_pages, 4)
    cache_spec = pl.BlockSpec((1, block_pages * PAGE, KVH * HD), lambda i, *_: (0, i, 0))
    whole_spec = pl.BlockSpec((group_size, HQ, HD), lambda i, *_: (0, 0, 0))
    shape = jax.ShapeDtypeStruct((group_size, HQ, HD), jnp.float32)
    return pl.pallas_call(
        functools.partial(attend_pages, block_pages),
        grid_spec=pltpu.PrefetchScalarGridSpec(
            num_scalar_prefetch=2,
            grid=(pool_pages // block_pages,),
            in_specs=[
                pl.BlockSpec(rows.shape, lambda i, *_: (0, 0, 0)),
                cache_spec,
                cache_spec,
            ],
            out_specs=[whole_spec, whole_spec],
        ),
        out_shape=[shape, shape],
        compiler_params=pltpu.CompilerParams(
            dimension_semantics=("arbitrary",), vmem_limit_bytes=40 * 1024 * 1024
        ),
        cost_estimate=pl.CostEstimate(
            flops=4 * pool_pages * HQ * PAGE * KVH * HD,
            bytes_accessed=4 * pool_pages * PAGE * KVH * HD,
            transcendentals=pool_pages * HQ * PAGE,
        ),
    )(owner, live, rows, k_cache, v_cache)


def shards(hidden, w_qkv, b_qkv, w_out, k_cache, v_cache, lengths, page_table, positions, group_of):
    seq_count = lax.axis_size("seq")
    grp_count = lax.axis_size("grp")
    seq_index = lax.axis_index("seq")
    grp_index = lax.axis_index("grp")
    request_total = group_of.shape[0]
    group_size = request_total // grp_count
    share = group_size // seq_count
    col_count = w_qkv.shape[1]
    col_start = grp_index * col_count
    turned = (HQ + KVH) * HD
    group_q = HQ // KVH
    score_scale = HD ** (-0.5)
    request_ids = jnp.arange(request_total, dtype=jnp.int32)
    before = (group_of[None, :] < group_of[:, None]) | (group_of[None, :] == group_of[:, None]) & (
        request_ids[None, :] < request_ids[:, None]
    )
    restore = jnp.sum(before.astype(jnp.int32), axis=1)
    placed_at = restore[None, :] == request_ids[:, None]
    served_order = jnp.sum(jnp.where(placed_at, request_ids[None, :], 0), axis=1)
    served_ids = lax.dynamic_slice_in_dim(served_order, grp_index * group_size, group_size, 0)
    send_order = (
        served_order.reshape(grp_count, seq_count, share).transpose(1, 0, 2).reshape(request_total)
    )
    hidden_all = lax.all_gather(hidden, "grp", axis=0, tiled=True)[send_order]
    partial_sum = jnp.dot(hidden_all, w_qkv, preferred_element_type=jnp.float32)
    summed = lax.psum_scatter(partial_sum, "seq", scatter_dimension=0, tiled=True)
    row_share = request_total // seq_count
    my_rows = lax.dynamic_slice_in_dim(send_order, seq_index * row_share, row_share, 0)
    fresh_rows = rotate_heads(
        summed + b_qkv[None, :], positions[:, my_rows], col_start, HD, turned
    ).astype(jnp.bfloat16)
    outgoing = fresh_rows.reshape(grp_count, share, col_count)
    incoming = lax.all_to_all(outgoing, "grp", split_axis=0, concat_axis=2, tiled=True)
    head_rows = incoming.reshape(share, grp_count * col_count // HD, HD)
    rows = lax.all_gather(head_rows, "seq", axis=0, tiled=True)

    served_len = lengths[served_ids]
    served_table = page_table[served_ids]
    most_pages = page_table.shape[1]
    page_counts = (served_len + PAGE - 1) // PAGE
    logical = jnp.arange(most_pages, dtype=jnp.int32)
    pool_pages = k_cache.shape[1] // PAGE
    local_page = served_table - seq_index * pool_pages
    usable = (
        (logical[None, :] < page_counts[:, None]) & (local_page >= 0) & (local_page < pool_pages)
    )
    pool_ids = jnp.arange(pool_pages, dtype=jnp.int32)
    matched = usable[:, :, None] & (local_page[:, :, None] == pool_ids[None, None, :])
    owner_ids = jnp.arange(group_size, dtype=jnp.int32)
    left = served_len[:, None] - logical[None, :] * PAGE
    live = jnp.max(jnp.where(matched, left[:, :, None], 0), axis=(0, 1))
    owner = jnp.max(jnp.where(matched, owner_ids[:, None, None], 0), axis=(0, 1))
    local_out, local_stat = local_attention(owner, live, rows, k_cache, v_cache)

    head_share = HQ // seq_count
    head_start = seq_index * head_share
    kv_share = max(1, head_share // group_q)
    kv_start = head_start // group_q
    query_here = lax.dynamic_slice_in_dim(rows, head_start, head_share, 1).astype(jnp.float32)
    key_here = lax.dynamic_slice_in_dim(rows, HQ + kv_start, kv_share, 1).astype(jnp.float32)
    value_here = lax.dynamic_slice_in_dim(rows, HQ + KVH + kv_start, kv_share, 1).astype(
        jnp.float32
    )
    key_here = jnp.repeat(key_here, head_share // kv_share, axis=1)
    value_here = jnp.repeat(value_here, head_share // kv_share, axis=1)
    new_here = jnp.sum(query_here * key_here, axis=2) * score_scale

    out_parts = lax.all_to_all(
        local_out.astype(jnp.bfloat16)
        .reshape(group_size, seq_count, head_share * HD)
        .transpose(1, 0, 2),
        "seq",
        split_axis=0,
        concat_axis=0,
        tiled=True,
    )
    stats = jnp.stack([local_stat[:, :, 0], local_stat[:, :, HD // 2]], axis=0)
    stats = stats.reshape(2, group_size, seq_count, head_share).transpose(2, 0, 1, 3)
    stat_parts = lax.all_to_all(
        stats.reshape(seq_count, 2 * group_size * head_share),
        "seq",
        split_axis=0,
        concat_axis=0,
        tiled=True,
    ).reshape(seq_count, 2, group_size, head_share)
    part_max = stat_parts[:, 0]
    part_total = stat_parts[:, 1]
    peak_here = jnp.maximum(jnp.max(part_max, axis=0), new_here)
    factor = jnp.exp(part_max - peak_here[None])
    fresh_weight = jnp.exp(new_here - peak_here)
    denominator = jnp.sum(part_total * factor, axis=0) + fresh_weight

    def widen(small):
        return jnp.repeat(small, HD, axis=-1)

    numerator = jnp.sum(out_parts.astype(jnp.float32) * widen(factor), axis=0) + widen(
        fresh_weight
    ) * value_here.reshape(group_size, head_share * HD)
    attended = (numerator / widen(denominator)).astype(jnp.bfloat16)
    gathered = lax.all_gather(attended, "grp", axis=0, tiled=True)
    by_request = gathered[restore]
    mixed = jnp.dot(by_request, w_out, preferred_element_type=jnp.float32).astype(jnp.bfloat16)
    mixed_parts = lax.all_to_all(
        mixed.reshape(seq_count, row_share, mixed.shape[1]),
        "seq",
        split_axis=0,
        concat_axis=0,
        tiled=True,
    )
    return jnp.sum(mixed_parts.astype(jnp.float32), axis=0).astype(jnp.bfloat16)


def solution(mesh):
    placed = (
        P("grp", "seq"),
        P("seq", "grp"),
        P("grp"),
        P("seq", "grp"),
        P("grp", "seq", None),
        P("grp", "seq", None),
        P(),
        P(),
        P(),
        P(),
    )
    return jax.shard_map(
        shards, mesh=mesh, in_specs=placed, out_specs=P("seq", "grp"), check_vma=False
    )
```

```python
import functools
import math

import jax
import jax.numpy as jnp
from jax import lax
from jax.experimental import pallas as pl
from jax.experimental.pallas import tpu as pltpu
from jax.sharding import PartitionSpec as P

HQ = 64
KVH = 8
HD = 128
PAGE = 128


rope_base = 1000000.0
neg_fill = -1e30


def rotate_heads(values, places, col_start, head_dim, turned):
    row_count, col_count = values.shape
    columns = col_start + jnp.arange(col_count, dtype=jnp.int32)
    within = columns % head_dim
    freq_index = within % (head_dim // 2)
    inverse_freq = jnp.exp(freq_index.astype(jnp.float32) * (-2.0 * math.log(rope_base) / head_dim))
    section = jnp.where(
        freq_index < head_dim // 8,
        0,
        jnp.where(freq_index < head_dim // 8 + 3 * head_dim // 16, 1, 2),
    )
    place_float = places.astype(jnp.float32)
    chosen = jnp.where(
        section[None, :] == 0,
        place_float[0][:, None],
        jnp.where(section[None, :] == 1, place_float[1][:, None], place_float[2][:, None]),
    )
    angles = chosen * inverse_freq[None, :]
    half = head_dim // 2
    partner = jnp.where(
        (within < half)[None, :], -jnp.roll(values, -half, axis=1), jnp.roll(values, half, axis=1)
    )
    rotated = values * jnp.cos(angles) + partner * jnp.sin(angles)
    return jnp.where((columns < turned)[None, :], rotated, values)


def attend_pages(block_pages, owner_ref, live_ref, rows_ref, key_ref, value_ref, out_ref, stat_ref):
    step = pl.program_id(0)
    group_q = HQ // KVH
    width = KVH * HD

    @pl.when(step == 0)
    def _():
        out_ref[...] = jnp.zeros_like(out_ref)
        lanes = lax.broadcasted_iota(jnp.int32, stat_ref.shape, 2)
        stat_ref[...] = jnp.where(lanes < HD // 2, neg_fill, 0.0)

    row_head = lax.broadcasted_iota(jnp.int32, (HQ, width), 0) // group_q
    col_head = lax.broadcasted_iota(jnp.int32, (HQ, width), 1) // HD
    own_head = (row_head == col_head).astype(jnp.float32).astype(jnp.bfloat16)
    place = lax.broadcasted_iota(jnp.int32, (HQ, PAGE), 1)
    lane = lax.broadcasted_iota(jnp.int32, (HQ, HD), 1)
    pages = []
    for j in range(block_pages):
        owner = owner_ref[step * block_pages + j]
        alive = place < live_ref[step * block_pages + j]
        query = rows_ref[owner, :HQ, :]
        spread = jnp.concatenate([query] * KVH, axis=1) * own_head
        keys = key_ref[0, j * PAGE : (j + 1) * PAGE, :]
        values = value_ref[0, j * PAGE : (j + 1) * PAGE, :]
        scores = lax.dot_general(
            spread, keys, (((1,), (1,)), ((), ())), preferred_element_type=jnp.float32
        ) * (HD**-0.5)
        scores = jnp.where(alive, scores, neg_fill)
        page_max = jnp.max(scores, axis=1, keepdims=True)
        weights = jnp.where(alive, jnp.exp(scores - page_max), 0.0)
        page_total = jnp.sum(weights, axis=1, keepdims=True)
        wide = jnp.dot(weights.astype(jnp.bfloat16), values, preferred_element_type=jnp.float32)
        page_out = jnp.concatenate(
            [
                wide[h * group_q : (h + 1) * group_q, h * HD : (h + 1) * HD]
                for h in range(KVH)
            ],
            axis=0,
        )
        pages.append((owner, page_max, page_total, page_out))
    for owner, page_max, page_total, page_out in pages:
        stat = stat_ref[owner]
        old_max = stat[:, :1]
        new_max = jnp.maximum(old_max, page_max)
        kept = jnp.exp(old_max - new_max)
        added = jnp.exp(page_max - new_max)
        out_ref[owner] = out_ref[owner] * kept + page_out * added
        total = stat[:, HD // 2 : HD // 2 + 1] * kept + page_total * added
        stat_ref[owner] = jnp.where(lane < HD // 2, new_max, total)


def local_attention(owner, live, rows, k_cache, v_cache):
    group_size = rows.shape[0]
    pool_pages = k_cache.shape[1] // PAGE
    block_pages = math.gcd(pool_pages, 4)
    cache_spec = pl.BlockSpec((1, block_pages * PAGE, KVH * HD), lambda i, *_: (0, i, 0))
    whole_spec = pl.BlockSpec((group_size, HQ, HD), lambda i, *_: (0, 0, 0))
    shape = jax.ShapeDtypeStruct((group_size, HQ, HD), jnp.float32)
    return pl.pallas_call(
        functools.partial(attend_pages, block_pages),
        grid_spec=pltpu.PrefetchScalarGridSpec(
            num_scalar_prefetch=2,
            grid=(pool_pages // block_pages,),
            in_specs=[
                pl.BlockSpec(rows.shape, lambda i, *_: (0, 0, 0)),
                cache_spec,
                cache_spec,
            ],
            out_specs=[whole_spec, whole_spec],
        ),
        out_shape=[shape, shape],
        compiler_params=pltpu.CompilerParams(
            dimension_semantics=("arbitrary",), vmem_limit_bytes=58 * 1024 * 1024
        ),
        cost_estimate=pl.CostEstimate(
            flops=4 * pool_pages * HQ * PAGE * KVH * HD,
            bytes_accessed=4 * pool_pages * PAGE * KVH * HD,
            transcendentals=pool_pages * HQ * PAGE,
        ),
    )(owner, live, rows, k_cache, v_cache)


def shards(hidden, w_qkv, b_qkv, w_out, k_cache, v_cache, lengths, page_table, positions, group_of):
    seq_count = lax.axis_size("seq")
    grp_count = lax.axis_size("grp")
    seq_index = lax.axis_index("seq")
    grp_index = lax.axis_index("grp")
    request_total = group_of.shape[0]
    group_size = request_total // grp_count
    share = group_size // seq_count
    col_count = w_qkv.shape[1]
    col_start = grp_index * col_count
    turned = (HQ + KVH) * HD
    group_q = HQ // KVH
    score_scale = HD ** (-0.5)
    request_ids = jnp.arange(request_total, dtype=jnp.int32)
    before = (group_of[None, :] < group_of[:, None]) | (group_of[None, :] == group_of[:, None]) & (
        request_ids[None, :] < request_ids[:, None]
    )
    restore = jnp.sum(before.astype(jnp.int32), axis=1)
    placed_at = restore[None, :] == request_ids[:, None]
    served_order = jnp.sum(jnp.where(placed_at, request_ids[None, :], 0), axis=1)
    served_ids = lax.dynamic_slice_in_dim(served_order, grp_index * group_size, group_size, 0)
    send_order = (
        served_order.reshape(grp_count, seq_count, share).transpose(1, 0, 2).reshape(request_total)
    )
    hidden_all = lax.all_gather(hidden, "grp", axis=0, tiled=True)[send_order]
    partial_sum = jnp.dot(hidden_all, w_qkv, preferred_element_type=jnp.float32)
    row_share = request_total // seq_count
    summed = jnp.sum(
        lax.all_to_all(
            partial_sum.reshape(seq_count, row_share, col_count),
            "seq",
            split_axis=0,
            concat_axis=0,
            tiled=True,
        ),
        axis=0,
    )
    my_rows = lax.dynamic_slice_in_dim(send_order, seq_index * row_share, row_share, 0)
    fresh_rows = rotate_heads(
        summed + b_qkv[None, :], positions[:, my_rows], col_start, HD, turned
    ).astype(jnp.bfloat16)
    outgoing = fresh_rows.reshape(grp_count, share, col_count)
    incoming = lax.all_to_all(outgoing, "grp", split_axis=0, concat_axis=2, tiled=True)
    head_rows = incoming.reshape(share, grp_count * col_count // HD, HD)
    rows = lax.all_to_all(
        jnp.broadcast_to(head_rows[None], (seq_count,) + head_rows.shape),
        "seq",
        split_axis=0,
        concat_axis=0,
        tiled=True,
    ).reshape((group_size,) + head_rows.shape[1:])

    served_len = lengths[served_ids]
    served_table = page_table[served_ids]
    most_pages = page_table.shape[1]
    page_counts = (served_len + PAGE - 1) // PAGE
    logical = jnp.arange(most_pages, dtype=jnp.int32)
    pool_pages = k_cache.shape[1] // PAGE
    local_page = served_table - seq_index * pool_pages
    usable = (
        (logical[None, :] < page_counts[:, None]) & (local_page >= 0) & (local_page < pool_pages)
    )
    pool_ids = jnp.arange(pool_pages, dtype=jnp.int32)
    matched = usable[:, :, None] & (local_page[:, :, None] == pool_ids[None, None, :])
    owner_ids = jnp.arange(group_size, dtype=jnp.int32)
    left = served_len[:, None] - logical[None, :] * PAGE
    live = jnp.max(jnp.where(matched, left[:, :, None], 0), axis=(0, 1))
    owner = jnp.max(jnp.where(matched, owner_ids[:, None, None], 0), axis=(0, 1))
    local_out, local_stat = local_attention(owner, live, rows, k_cache, v_cache)

    head_share = HQ // seq_count
    head_start = seq_index * head_share
    kv_share = max(1, head_share // group_q)
    kv_start = head_start // group_q
    query_here = lax.dynamic_slice_in_dim(rows, head_start, head_share, 1).astype(jnp.float32)
    key_here = lax.dynamic_slice_in_dim(rows, HQ + kv_start, kv_share, 1).astype(jnp.float32)
    value_here = lax.dynamic_slice_in_dim(rows, HQ + KVH + kv_start, kv_share, 1).astype(
        jnp.float32
    )
    key_here = jnp.repeat(key_here, head_share // kv_share, axis=1)
    value_here = jnp.repeat(value_here, head_share // kv_share, axis=1)
    new_here = jnp.sum(query_here * key_here, axis=2) * score_scale

    out_parts = lax.all_to_all(
        local_out.astype(jnp.bfloat16)
        .reshape(group_size, seq_count, head_share * HD)
        .transpose(1, 0, 2),
        "seq",
        split_axis=0,
        concat_axis=0,
        tiled=True,
    )
    stats = jnp.stack([local_stat[:, :, 0], local_stat[:, :, HD // 2]], axis=0)
    stats = stats.reshape(2, group_size, seq_count, head_share).transpose(2, 0, 1, 3)
    stat_parts = lax.all_to_all(
        stats.reshape(seq_count, 2 * group_size * head_share),
        "seq",
        split_axis=0,
        concat_axis=0,
        tiled=True,
    ).reshape(seq_count, 2, group_size, head_share)
    part_max = stat_parts[:, 0]
    part_total = stat_parts[:, 1]
    peak_here = jnp.maximum(jnp.max(part_max, axis=0), new_here)
    factor = jnp.exp(part_max - peak_here[None])
    fresh_weight = jnp.exp(new_here - peak_here)
    denominator = jnp.sum(part_total * factor, axis=0) + fresh_weight

    def widen(small):
        return jnp.repeat(small, HD, axis=-1)

    numerator = jnp.sum(out_parts.astype(jnp.float32) * widen(factor), axis=0) + widen(
        fresh_weight
    ) * value_here.reshape(group_size, head_share * HD)
    attended = (numerator / widen(denominator)).astype(jnp.bfloat16)
    gathered = lax.all_gather(attended, "grp", axis=0, tiled=True)
    by_request = gathered[restore]
    mixed = jnp.dot(by_request, w_out, preferred_element_type=jnp.float32).astype(jnp.bfloat16)
    mixed_parts = lax.all_to_all(
        mixed.reshape(seq_count, row_share, mixed.shape[1]),
        "seq",
        split_axis=0,
        concat_axis=0,
        tiled=True,
    )
    return jnp.sum(mixed_parts.astype(jnp.float32), axis=0).astype(jnp.bfloat16)


def solution(mesh):
    placed = (
        P("grp", "seq"),
        P("seq", "grp"),
        P("grp"),
        P("seq", "grp"),
        P("grp", "seq", None),
        P("grp", "seq", None),
        P(),
        P(),
        P(),
        P(),
    )
    return jax.shard_map(
        shards, mesh=mesh, in_specs=placed, out_specs=P("seq", "grp"), check_vma=False
    )
```
